32 devices in a mesh: gx: 8 (over y, x, core), gy: 4 (over z).
Axes of the slice: x: 2, y: 2, z: 4, core: 2. Of those that a mesh axis runs over, the one named last changes fastest.
Arguments:
- source_field: bfloat16 [4096, 128, 128], P(('gx', 'gy')), may hold values from -6 to 6
- weight_blocks: bfloat16 [16384, 128, 128], P(('gx', 'gy')), may hold values from -0.1875 to 0.1875
- source_ids: int32 [16384], replicated, may hold values from 0 to 4095, as said below
- target_ids: int32 [16384], replicated, may hold values from 0 to 2047, as said below
Outputs:
- remapped: bfloat16 [2048, 128, 128], P(('gx', 'gy'))
The draws below stay inside these ranges and needn't reach their ends.
Inputs may be any that keep to these rules, and one draw needn't show every extreme that they name: `source_ids`: source block b lies on device b // 128 of gx+gy, and weight block k lies on device k // 512. The weight blocks of device d name only source blocks of devices d - 2 to d + 2. Among the weight blocks of one device, at most 64 distinct source blocks of any one other device are named, and exactly 64 for some other device. `target_ids`: target block t lies on device t // 64 of gx+gy. The weight blocks of device d name only target blocks of devices d - 2 to d + 2. Among the weight blocks of one device, at most 16 distinct target blocks of any one device are named, and exactly 16 for some other device.
All inputs are finite; a program needn't handle non-finite values.
Results may differ from the reference program's by a relative error of at most 0.001.
Values may be sent and summed in bfloat16 or wider, within the bound.
A program may use at most 192 MiB of HBM per device.

```python
import jax
import jax.numpy as jnp
from jax import lax

BLK = 128
CH = 128
HALF = 2
SB_DEV = 128
TB_DEV = 64
WB_DEV = 512
CAP_S = 64
CAP_T = 16
NSB = 4096
NW = 16384
N_GX = 8
N_GY = 4


def pair_ids(key, slot_count, per_device):
    devices = N_GX * N_GY
    span = 2 * HALF + 1

    def one_device(device):
        keyed = jax.random.fold_in(key, device)
        key_count, key_force, key_perm, key_pick, key_order = jax.random.split(keyed, 5)
        offsets = jnp.arange(span, dtype=jnp.int32) - HALF
        owner = device + offsets
        valid = (owner >= 0) & (owner < devices)
        counts = jax.random.randint(key_count, (span,), slot_count // 2, slot_count + 1)
        scores = jax.random.randint(key_force, (span,), 0, 1024) * span + jnp.arange(span, dtype=jnp.int32)
        scores = jnp.where(valid & (offsets != 0), scores, -1)
        forced = jnp.argmax(scores)
        counts = jnp.where((jnp.arange(span, dtype=jnp.int32) == forced) | (offsets == 0), slot_count, counts)
        counts = jnp.where(valid, counts, 0)
        perms = jax.vmap(lambda kk: jax.random.permutation(kk, per_device))(jax.random.split(key_perm, span))
        chosen = perms[:, :slot_count].reshape(-1)
        used = (jnp.arange(slot_count, dtype=jnp.int32)[None, :] < counts[:, None]).reshape(-1)
        entries = span * slot_count
        block_index = jnp.arange(WB_DEV, dtype=jnp.int32)
        picked = jax.random.randint(key_pick, (WB_DEV,), 0, entries)
        entry = jnp.where(block_index < entries, block_index, picked)
        entry = jnp.where(used[entry], entry, HALF * slot_count + entry % slot_count)
        order = jax.random.permutation(key_order, WB_DEV)
        entry = entry[order]
        return (owner[entry // slot_count] * per_device + chosen[entry]).astype(jnp.int32)
    return jax.vmap(one_device)(jnp.arange(devices, dtype=jnp.int32)).reshape(-1).astype(jnp.int32)


def draw_source_ids(key, part):
    return pair_ids(jax.random.fold_in(key, 11), CAP_S, SB_DEV)


def draw_target_ids(key, part):
    return pair_ids(jax.random.fold_in(key, 23), CAP_T, TB_DEV)


def shard_levels(stream_key, shape, pieces, least, largest):
    gain = 1.0
    for dim, parts in pieces:
        draws = jax.random.uniform(jax.random.fold_in(jax.random.fold_in(stream_key, 6), dim), (parts,), jnp.float32, least / len(pieces), largest / len(pieces))
        gain = gain * jnp.repeat(jnp.exp(draws), shape[dim] // parts).reshape((-1,) + (1,) * (len(shape) - 1 - dim))
    return gain


def centred(own_key, shape, scale, most, cuts=(), kind=jnp.bfloat16):
    gain = shard_levels(own_key, shape, cuts, -0.22, 0.18) if cuts else 1.0
    array = jax.random.normal(own_key, shape, jnp.float32) * scale * gain
    return jnp.minimum(jnp.maximum(array, -most), most).astype(kind)


def setup_inputs(seed: int = 0) -> dict:
    splits = jax.random.split(jax.random.key(seed), 5)
    return {
        "source_field": centred(splits[0], (NSB, BLK, CH), 1.0, 6.0, ((0, 32),)),
        "weight_blocks": centred(splits[1], (NW, BLK, BLK), (BLK * WB_DEV // TB_DEV) ** -0.5, 0.1875, ((0, 32),)),
        "source_ids": draw_source_ids(jax.random.fold_in(splits[4], 71), 0),
        "target_ids": draw_target_ids(jax.random.fold_in(splits[4], 71), 0),
    }


def reference(source_field, weight_blocks, source_ids, target_ids):
    devices = N_GX * N_GY
    total = jnp.zeros((TB_DEV * devices, BLK, CH), jnp.float32)

    def accumulate(carry, index):
        start = (index * WB_DEV).astype(jnp.int32)
        weights = lax.dynamic_slice_in_dim(weight_blocks, start, WB_DEV, 0)
        src_rows = lax.dynamic_slice_in_dim(source_ids, start, WB_DEV, 0)
        tgt_rows = lax.dynamic_slice_in_dim(target_ids, start, WB_DEV, 0)
        gathered = source_field[src_rows]
        partial_value = jnp.einsum("kts,ksc->ktc", weights.astype(jnp.float32), gathered.astype(jnp.float32))
        return carry.at[tgt_rows].add(partial_value), None

    total, _ = lax.scan(accumulate, total, jnp.arange(devices, dtype=jnp.int32))
    return total.astype(jnp.bfloat16)
```

```python
import functools

import jax
import jax.numpy as jnp
from jax import lax
from jax.experimental import pallas as pl
from jax.experimental.pallas import tpu as pltpu
from jax.sharding import PartitionSpec as P

HALF = 2
TB_DEV = 64
CAP_S = 64
CAP_T = 16
SPAN = 2 * HALF + 1
AXES = ("gx", "gy")
MESH = pl.DeviceIdType.MESH
QUAD = 4
CHUNK = 4
GROUP = 8
TILE = 128
LOW_EXPONENT = -110.0


def passed_along(value, steps):
    count = lax.axis_size(AXES)
    initial, last = (max(0, -steps), min(count, count - steps))
    return lax.ppermute(value, AXES, [(source, source + steps) for source in range(initial, last)])


def rows_of(ids, device, devices, held):
    clamped = jnp.clip(device, 0, devices - 1)
    return lax.dynamic_slice_in_dim(ids, clamped * held, held, 0)


def named(rows, low, count):
    return jnp.any(rows[:, None] == low + jnp.arange(count, dtype=jnp.int32)[None, :], axis=0)


def ranks_of(asked):
    count = asked.shape[1]
    before = jnp.arange(count)[:, None] < jnp.arange(count)[None, :]
    return jnp.sum((asked[:, :, None] & before[None]).astype(jnp.int32), axis=1)


def exchange_kernel(devices, n_gy, sel, src, recv, srcv, hst, xst, lsem, rsem, ssem):
    nb = src.shape[0]
    pieces = nb // CHUNK
    half = CAP_S // CHUNK
    me = lax.axis_index("gx") * n_gy + lax.axis_index("gy")
    r = lax.rem(me, QUAD)
    inner = (r == 1) | (r == 2)
    outer = jnp.logical_not(inner)
    sgn = jnp.where(r < 2, 1, -1)
    partner = me + 1 - 2 * lax.rem(r, 2)
    near = me + sgn
    far = me + 2 * sgn
    to = me + QUAD * sgn
    source = me - QUAD * sgn
    has_to = (to >= 0) & (to < devices)
    has_from = (source >= 0) & (source < devices)
    base_a, base_b, base_c, base_h, base_o = 0, nb, 2 * nb, 3 * nb, 3 * nb + CAP_S

    def at(device):
        return (device // n_gy, lax.rem(device, n_gy))

    barrier = pltpu.get_barrier_semaphore()

    def greet(device):
        pl.semaphore_signal(barrier, inc=1, device_id=at(device), device_id_type=MESH)

    greet(partner)
    greet(far)
    pl.when(inner)(lambda: greet(near))
    pl.when(has_to)(lambda: greet(to))
    pl.when(has_from)(lambda: greet(source))
    peers = 2 + inner.astype(jnp.int32) + has_to.astype(jnp.int32) + has_from.astype(jnp.int32)
    pl.semaphore_wait(barrier, peers)

    def piece(base, k):
        return recv.at[pl.ds(base + k * CHUNK, CHUNK)]

    def copy(ref, base, k, send, got, device):
        return pltpu.make_async_remote_copy(
            src_ref=ref,
            dst_ref=piece(base, k),
            send_sem=ssem.at[send, k],
            recv_sem=rsem.at[got, k],
            device_id=at(device),
            device_id_type=MESH,
        )

    def cross_inner(k):
        return copy(src.at[pl.ds(k * CHUNK, CHUNK)], base_a, k, 0, 0, near)

    def cross_outer(k):
        return copy(xst.at[pl.ds(k * CHUNK, CHUNK)], base_b, k, 0, 1, far)

    def side(k):
        return copy(hst.at[pl.ds(k * CHUNK, CHUNK)], base_h, k, 1, 3, partner)

    def ahead(k):
        return copy(piece(base_a, k), base_a, k, 2, 0, partner)

    def over_outer(k):
        return copy(piece(base_a, k), base_b, k, 3, 1, to)

    def over_inner(k):
        return copy(piece(base_b, k), base_c, k, 3, 2, to)

    def last(k):
        return copy(piece(base_c, k), base_c, k, 4, 2, partner)

    def await_piece(base, got, k):
        copy(piece(base, k), base, k, 0, got, partner).wait_recv()

    @pl.when(inner)
    def _():
        for k in range(pieces):
            cross_inner(k).start()

    load = pltpu.make_async_copy(src, srcv, lsem.at[0])
    keep = pltpu.make_async_copy(src, recv.at[pl.ds(base_o, nb)], lsem.at[1])
    load.start()
    keep.start()
    load.wait()

    def pick_side(j, carry):
        hst[j] = srcv[sel[j]]
        return carry

    lax.fori_loop(0, CAP_S, pick_side, 0)

    @pl.when(outer)
    def _():
        def pick(j, carry):
            xst[j] = srcv[sel[CAP_S + j]]
            return carry

        lax.fori_loop(0, nb, pick, 0)

    keep.wait()

    @pl.when(inner)
    def _():
        for k in range(half):
            side(k).start()

    @pl.when(outer)
    def _():
        for k in range(pieces):
            cross_outer(k).start()
        for k in range(half):
            side(k).start()
        for k in range(pieces):
            await_piece(base_a, 0, k)

            @pl.when(has_to)
            def _():
                over_outer(k).start()

        @pl.when(has_from)
        def _():
            for k in range(pieces):
                await_piece(base_b, 1, k)
            for k in range(half):
                await_piece(base_c, 2, k)

        for k in range(pieces):
            cross_outer(k).wait_send()

        @pl.when(has_to)
        def _():
            for k in range(pieces):
                over_outer(k).wait_send()

    @pl.when(inner)
    def _():
        def from_far(k):
            await_piece(base_b, 1, k)

            @pl.when(has_to)
            def _():
                over_inner(k).start()

        def from_shift(k):
            if 0 <= k < half:

                @pl.when(has_from)
                def _():
                    await_piece(base_c, 2, k)
                    last(k).start()

        for k in range(pieces):
            from_far(k)
            from_shift(k - 1)
        for k in range(pieces):
            await_piece(base_a, 0, k)
            ahead(k).start()

        @pl.when(has_from)
        def _():
            for k in range(half, pieces):
                await_piece(base_c, 2, k)
            for k in range(half):
                last(k).wait_send()

        for k in range(pieces):
            cross_inner(k).wait_send()
            ahead(k).wait_send()

        @pl.when(has_to)
        def _():
            for k in range(pieces):
                over_inner(k).wait_send()

    for k in range(half):
        await_piece(base_h, 3, k)
        side(k).wait_send()


def exchange_call(n_gy, devices, sel, source_field):
    nb = source_field.shape[0]
    tile = source_field.shape[1:]
    kind = source_field.dtype
    pieces = nb // CHUNK
    return pl.pallas_call(
        functools.partial(exchange_kernel, devices, n_gy),
        out_shape=jax.ShapeDtypeStruct((4 * nb + CAP_S,) + tile, kind),
        in_specs=[pl.BlockSpec(memory_space=pltpu.SMEM), pl.BlockSpec(memory_space=pltpu.HBM)],
        out_specs=pl.BlockSpec(memory_space=pltpu.VMEM),
        scratch_shapes=[
            pltpu.VMEM((nb,) + tile, kind),
            pltpu.VMEM((CAP_S,) + tile, kind),
            pltpu.VMEM((nb,) + tile, kind),
            pltpu.SemaphoreType.DMA((2,)),
            pltpu.SemaphoreType.DMA((4, pieces)),
            pltpu.SemaphoreType.DMA((5, pieces)),
        ],
        name="exchange",
        compiler_params=pltpu.CompilerParams(
            collective_id=0, has_side_effects=True, vmem_limit_bytes=12 * 2**20
        ),
    )(sel, source_field)


def products_kernel(group, bounds, packed, weights, src, *refs):
    own = group == 2
    outs, acc = refs[:-1], refs[-1]
    first = bounds[group]
    rounds = (bounds[group + 1] - first) // GROUP
    acc[...] = jnp.zeros_like(acc)

    def run(g, carry):
        items = [packed[first + g * GROUP + u] for u in range(GROUP)]
        sums = []
        for item in items:
            k, s = lax.shift_right_logical(item, 16), lax.shift_right_logical(item, 6) & 1023
            sums.append(jnp.dot(weights[k], src[s], preferred_element_type=jnp.float32))
        for item, value in zip(items, sums):
            acc[item & 63] += value
        return carry

    lax.fori_loop(0, rounds, run, 0)

    if own:
        outs[0][...] = acc[1 : 1 + CAP_T]
        return
    rows = lax.broadcasted_iota(jnp.int32, (CAP_T, TILE), 0)
    for r in range(2):

        def encode(b, exponents, r=r):
            value = acc[1 + r * CAP_T + b]
            most = jnp.max(jnp.abs(value), axis=0, keepdims=True)
            exponent = jnp.ceil(jnp.log(jnp.maximum(most, 1e-37)) * 1.4426950408889634)
            exponent = jnp.maximum(exponent, LOW_EXPONENT)
            scaled = jnp.floor(value * jnp.exp2(15.0 - exponent) + 0.5)
            scaled = jnp.clip(scaled, -32767.0, 32767.0)
            outs[r][pl.ds(pl.multiple_of(b * TILE, TILE), TILE), :] = scaled.astype(jnp.int32).astype(jnp.int16)
            return jnp.where(rows == b, exponent.astype(jnp.int32), exponents)

        exponents = lax.fori_loop(0, CAP_T, encode, jnp.zeros((CAP_T, TILE), jnp.int32))
        outs[r][CAP_T * TILE :, :] = exponents.astype(jnp.int16)


def products_call(group, bounds, packed, weights, src):
    own = group == 2
    tile = weights.shape[1:2] + src.shape[2:]
    smem = pl.BlockSpec(memory_space=pltpu.SMEM)
    vmem = pl.BlockSpec(memory_space=pltpu.VMEM)
    slots = 1 + (1 if own else 2) * CAP_T
    if own:
        out_shape = [jax.ShapeDtypeStruct((CAP_T,) + tile, jnp.float32)]
    else:
        out_shape = [jax.ShapeDtypeStruct((CAP_T * tile[0] + CAP_T, tile[1]), jnp.int16)] * 2
    share = weights.shape[0] // 3
    return pl.pallas_call(
        functools.partial(products_kernel, group),
        out_shape=out_shape,
        in_specs=[smem, smem, vmem, vmem],
        out_specs=[vmem] * len(out_shape),
        scratch_shapes=[
            pltpu.VMEM((slots,) + tile, jnp.float32),
        ],
        name=f"products_{group}",
        cost_estimate=pl.CostEstimate(
            flops=share * 2 * 128**3, bytes_accessed=8 * 2**20, transcendentals=0
        ),
        compiler_params=pltpu.CompilerParams(vmem_limit_bytes=6 * 2**20),
    )(bounds, packed, weights, src)


def final_kernel(places, *refs):
    boxes, out = refs[:SPAN], refs[SPAN]
    scales = refs[SPAN + 1]
    for s in range(SPAN):
        if s != HALF:
            scales[s] = jnp.exp2(boxes[s][CAP_T * TILE :, :].astype(jnp.float32) - 15.0)

    def one(b, carry):
        total = jnp.zeros(out.shape[1:], jnp.float32)
        for s in range(SPAN):
            place = places[s * TB_DEV + b]
            slot = jnp.maximum(place, 0)
            if s == HALF:
                value = boxes[s][slot]
            else:
                rows = pl.ds(pl.multiple_of(slot * TILE, TILE), TILE)
                value = boxes[s][rows, :].astype(jnp.float32) * scales[s, pl.ds(slot, 1), :]
            total = total + jnp.where(place >= 0, value, 0.0)
        out[b] = total.astype(out.dtype)
        return carry

    lax.fori_loop(0, TB_DEV, one, 0)


def final_call(places, boxes):
    tile = boxes[HALF].shape[1:]
    vmem = pl.BlockSpec(memory_space=pltpu.VMEM)
    return pl.pallas_call(
        final_kernel,
        out_shape=jax.ShapeDtypeStruct((TB_DEV,) + tile, jnp.bfloat16),
        in_specs=[pl.BlockSpec(memory_space=pltpu.SMEM)] + [vmem] * SPAN,
        out_specs=vmem,
        scratch_shapes=[pltpu.VMEM((SPAN, CAP_T, tile[1]), jnp.float32)],
        name="final_sum",
        compiler_params=pltpu.CompilerParams(vmem_limit_bytes=32 * 2**20),
    )(places, *boxes)


def body(source_field, weight_blocks, source_ids, target_ids):
    devices = lax.axis_size(AXES)
    n_gy = lax.axis_size("gy")
    me = lax.axis_index(AXES)
    held = weight_blocks.shape[0]
    nb = source_field.shape[0]
    blocks = jnp.arange(nb, dtype=jnp.int32)
    r = me % QUAD

    def asked_by(device, owner):
        return named(rows_of(source_ids, device, devices, held), owner * nb, nb)

    def edge_of(owner):
        return jnp.where(owner % QUAD < 2, owner - 1, owner + 1)

    partner = me + 1 - 2 * (r % 2)
    asked = jnp.stack(
        [
            asked_by(partner, me),
            asked_by(edge_of(me), me),
            asked_by(edge_of(me - 2), me - 2),
            asked_by(edge_of(me + 2), me + 2),
        ]
    )
    ranks = ranks_of(asked)
    counts = jnp.sum(asked.astype(jnp.int32), axis=1, keepdims=True)
    orders = jnp.where(asked, ranks, counts + blocks[None, :] - ranks)
    chosen = jnp.sum(
        jnp.where(orders[:2, None, :] == blocks[None, :, None], blocks[None, None, :], 0), axis=2
    )
    sel = jnp.concatenate([chosen[0, :CAP_S], chosen[1]])
    recv = exchange_call(n_gy, devices, sel, source_field)

    base_a, base_b, base_c, base_h, base_o = 0, nb, 2 * nb, 3 * nb, 3 * nb + CAP_S
    own_src = rows_of(source_ids, me, devices, held)
    low = (me - HALF) * nb
    own_ranks = ranks_of(named(own_src, low, SPAN * nb).reshape(SPAN, nb))
    far_low, far_high = orders[2], orders[3]
    tables = [
        [base_b + blocks, base_c + own_ranks[1], base_o + blocks, base_h + own_ranks[3], base_a + blocks],
        [base_c + far_low, base_h + own_ranks[1], base_o + blocks, base_a + blocks, base_b + far_high],
        [base_b + far_low, base_a + blocks, base_o + blocks, base_h + own_ranks[3], base_c + far_high],
        [base_a + blocks, base_h + own_ranks[1], base_o + blocks, base_c + own_ranks[3], base_b + blocks],
    ]
    tables = [jnp.stack(rows) for rows in tables]
    table = jnp.where(
        r < 2, jnp.where(r == 0, tables[0], tables[1]), jnp.where(r == 2, tables[2], tables[3])
    ).reshape(-1)
    hits = (own_src - low)[:, None] == jnp.arange(SPAN * nb, dtype=jnp.int32)[None, :]
    place = jnp.sum(jnp.where(hits, table[None, :], 0), axis=1)

    own_tgt = rows_of(target_ids, me, devices, held)
    low = (me - HALF) * TB_DEV
    tgt_asked = named(own_tgt, low, SPAN * TB_DEV).reshape(SPAN, TB_DEV)
    steps = jnp.arange(SPAN, dtype=jnp.int32)[:, None] - HALF
    tgt_group = HALF - jnp.abs(steps)
    tgt_slot = 1 + ranks_of(tgt_asked) + jnp.where(steps > 0, CAP_T, 0)
    hits = (own_tgt - low)[:, None] == jnp.arange(SPAN * TB_DEV, dtype=jnp.int32)[None, :]
    marks = jnp.sum(jnp.where(hits, (tgt_slot + 64 * tgt_group).reshape(-1)[None, :], 0), axis=1)
    group, slot = marks // 64, marks % 64

    index = jnp.arange(held, dtype=jnp.int32)
    groups = jnp.arange(4, dtype=jnp.int32)
    sizes = jnp.sum((group[None, :] == groups[:, None]).astype(jnp.int32), axis=1)
    sizes = (sizes + GROUP - 1) // GROUP * GROUP
    bounds = jnp.sum(jnp.where(groups[None, :] < groups[:, None], sizes[None, :], 0), axis=1)
    earlier = (group[:, None] == group[None, :]) & (index[:, None] < index[None, :])
    position = jnp.sum(earlier.astype(jnp.int32), axis=0)
    position = position + jnp.sum(
        jnp.where(group[None, :] == groups[:, None], bounds[:, None], 0), axis=0
    )
    item = (index * 1024 + place) * 64 + slot
    spots = jnp.arange(held + 4 * GROUP, dtype=jnp.int32)
    packed = jnp.sum(jnp.where(position[None, :] == spots[:, None], item[None, :], 0), axis=1)

    box_asked = []
    for step in range(-HALF, HALF + 1):
        sender = me - step
        valid = (sender >= 0) & (sender < devices)
        rows = rows_of(target_ids, sender, devices, held)
        box_asked.append(named(rows, me * TB_DEV, TB_DEV) & valid)
    box_asked = jnp.stack(box_asked)
    places = jnp.where(box_asked, ranks_of(box_asked), -1).reshape(-1)

    boxes = [None] * SPAN
    for g, step in ((0, 2), (1, 1)):
        below, above = products_call(g, bounds, packed, weight_blocks, recv)
        bounds, below, above = lax.optimization_barrier((bounds, below, above))
        boxes[HALF - step] = passed_along(below, -step)
        boxes[HALF + step] = passed_along(above, step)
    (boxes[HALF],) = products_call(2, bounds, packed, weight_blocks, recv)
    return final_call(places, boxes)


def solution(mesh):
    return jax.shard_map(
        body,
        mesh=mesh,
        in_specs=(P(AXES, None, None), P(AXES, None, None), P(), P()),
        out_specs=P(AXES, None, None),
        check_vma=False,
    )
```

```python
import functools

import jax
import jax.numpy as jnp
from jax import lax
from jax.experimental import pallas as pl
from jax.experimental.pallas import tpu as pltpu
from jax.sharding import PartitionSpec as P


HALF = 2
TB_DEV = 64
CAP_S = 64
CAP_T = 16
SPAN = 2 * HALF + 1
AXES = ("gx", "gy")
MESH = pl.DeviceIdType.MESH
QUAD = 4
CHUNK = 4
GROUP = 8
TILE = 128
RARE = 12
LOW_EXPONENT = -110.0


def passed_along(value, steps):
    count = lax.axis_size(AXES)
    initial, last = (max(0, -steps), min(count, count - steps))
    return lax.ppermute(value, AXES, [(source, source + steps) for source in range(initial, last)])


def rows_of(ids, device, devices, held):
    clamped = jnp.clip(device, 0, devices - 1)
    return lax.dynamic_slice_in_dim(ids, clamped * held, held, 0)


def named(rows, low, count):
    return jnp.any(rows[:, None] == low + jnp.arange(count, dtype=jnp.int32)[None, :], axis=0)


def ranks_of(asked):
    count = asked.shape[1]
    before = jnp.arange(count)[:, None] < jnp.arange(count)[None, :]
    return jnp.sum((asked[:, :, None] & before[None]).astype(jnp.int32), axis=1)


def exchange_kernel(devices, n_gy, count, sel, src, recv, srcv, hst, xst, lsem, rsem, ssem):
    nb = src.shape[0]
    pieces = count // CHUNK
    half = CAP_S // CHUNK
    me = lax.axis_index("gx") * n_gy + lax.axis_index("gy")
    r = lax.rem(me, QUAD)
    inner = (r == 1) | (r == 2)
    outer = jnp.logical_not(inner)
    sgn = jnp.where(r < 2, 1, -1)
    partner = me + 1 - 2 * lax.rem(r, 2)
    near = me + sgn
    far = me + 2 * sgn
    to = me + QUAD * sgn
    source = me - QUAD * sgn
    has_to = (to >= 0) & (to < devices)
    has_from = (source >= 0) & (source < devices)
    base_a, base_b, base_c, base_h, base_o = 0, nb, 2 * nb, 3 * nb, 3 * nb + CAP_S

    def at(device):
        return (device // n_gy, lax.rem(device, n_gy))

    barrier = pltpu.get_barrier_semaphore()

    def greet(device):
        pl.semaphore_signal(barrier, inc=1, device_id=at(device), device_id_type=MESH)

    greet(partner)
    greet(far)
    pl.when(inner)(lambda: greet(near))
    pl.when(has_to)(lambda: greet(to))
    pl.when(has_from)(lambda: greet(source))
    peers = 2 + inner.astype(jnp.int32) + has_to.astype(jnp.int32) + has_from.astype(jnp.int32)
    pl.semaphore_wait(barrier, peers)

    def piece(base, k):
        return recv.at[pl.ds(base + k * CHUNK, CHUNK)]

    def copy(ref, base, k, send, got, device):
        return pltpu.make_async_remote_copy(
            src_ref=ref,
            dst_ref=piece(base, k),
            send_sem=ssem.at[send, k],
            recv_sem=rsem.at[got, k],
            device_id=at(device),
            device_id_type=MESH,
        )

    def cross_inner(k):
        return copy(xst.at[pl.ds(k * CHUNK, CHUNK)], base_a, k, 0, 0, near)

    def cross_outer(k):
        return copy(xst.at[pl.ds(k * CHUNK, CHUNK)], base_b, k, 0, 1, far)

    def side(k):
        return copy(hst.at[pl.ds(k * CHUNK, CHUNK)], base_h, k, 1, 3, partner)

    def ahead(k):
        return copy(piece(base_a, k), base_a, k, 2, 0, partner)

    def over_outer(k):
        return copy(piece(base_a, k), base_b, k, 3, 1, to)

    def over_inner(k):
        return copy(piece(base_b, k), base_c, k, 3, 2, to)

    def last(k):
        return copy(piece(base_c, k), base_c, k, 4, 2, partner)

    def await_piece(base, got, k):
        copy(piece(base, k), base, k, 0, got, partner).wait_recv()

    load = pltpu.make_async_copy(src, srcv, lsem.at[0])
    load.start()
    keep = pltpu.make_async_copy(src, recv.at[pl.ds(base_o, nb)], lsem.at[1])
    load.wait()

    def pick(j, carry):
        for u in range(CHUNK):
            xst[j * CHUNK + u] = srcv[sel[CAP_S + j * CHUNK + u]]
        return carry

    def pick_side(j, carry):
        for u in range(CHUNK):
            hst[j * CHUNK + u] = srcv[sel[j * CHUNK + u]]
        return carry

    lax.fori_loop(0, pieces, pick, 0)
    lax.fori_loop(0, half, pick_side, 0)

    @pl.when(inner)
    def _():
        for k in range(pieces):
            cross_inner(k).start()
        for k in range(half):
            side(k).start()

    keep.start()

    @pl.when(outer)
    def _():
        for k in range(pieces):
            cross_outer(k).start()
        for k in range(half):
            side(k).start()
        for k in range(pieces):
            await_piece(base_a, 0, k)

            @pl.when(has_to)
            def _():
                over_outer(k).start()

        @pl.when(has_from)
        def _():
            for k in range(pieces):
                await_piece(base_b, 1, k)
            for k in range(half):
                await_piece(base_c, 2, k)

        for k in range(pieces):
            cross_outer(k).wait_send()

        @pl.when(has_to)
        def _():
            for k in range(pieces):
                over_outer(k).wait_send()

    @pl.when(inner)
    def _():
        def from_far(k):
            await_piece(base_b, 1, k)

            @pl.when(has_to)
            def _():
                over_inner(k).start()

        def from_shift(k):
            if 0 <= k < half:

                @pl.when(has_from)
                def _():
                    await_piece(base_c, 2, k)
                    last(k).start()

        for k in range(pieces):
            from_far(k)
            from_shift(k - 1)
        for k in range(pieces):
            await_piece(base_a, 0, k)
            ahead(k).start()

        @pl.when(has_from)
        def _():
            for k in range(half, pieces):
                await_piece(base_c, 2, k)
            for k in range(half):
                last(k).wait_send()

        for k in range(pieces):
            cross_inner(k).wait_send()
            ahead(k).wait_send()

        @pl.when(has_to)
        def _():
            for k in range(pieces):
                over_inner(k).wait_send()

    for k in range(half):
        await_piece(base_h, 3, k)
        side(k).wait_send()
    keep.wait()


def exchange_call(n_gy, devices, rare, sel, source_field):
    nb = source_field.shape[0]
    tile = source_field.shape[1:]
    kind = source_field.dtype
    count = nb if rare else nb - RARE
    pieces = count // CHUNK
    anywhere = pl.BlockSpec(memory_space=pl.ANY)
    vmem = pl.BlockSpec(memory_space=pltpu.VMEM)
    return pl.pallas_call(
        functools.partial(exchange_kernel, devices, n_gy, count),
        out_shape=jax.ShapeDtypeStruct((4 * nb + CAP_S,) + tile, kind),
        in_specs=[pl.BlockSpec(memory_space=pltpu.SMEM), anywhere],
        out_specs=anywhere if rare else vmem,
        scratch_shapes=[
            pltpu.VMEM((nb,) + tile, kind),
            pltpu.VMEM((CAP_S,) + tile, kind),
            pltpu.VMEM((count,) + tile, kind),
            pltpu.SemaphoreType.DMA((3,)),
            pltpu.SemaphoreType.DMA((4, pieces)),
            pltpu.SemaphoreType.DMA((5, pieces)),
        ],
        name="exchange_all" if rare else "exchange",
        cost_estimate=pl.CostEstimate(flops=2 * 10**10, bytes_accessed=8 * 2**20, transcendentals=0),
        compiler_params=pltpu.CompilerParams(
            collective_id=int(rare), has_side_effects=True, vmem_limit_bytes=12 * 2**20
        ),
    )(sel, source_field)


def products_kernel(groups, bounds, packed, weights, pool, *refs):
    outs, acc = refs[:-1], refs[-1]
    rows = lax.broadcasted_iota(jnp.int32, (CAP_T, TILE), 0)
    for group in groups:
        first = bounds[group]
        rounds = (bounds[group + 1] - first) // GROUP
        acc[...] = jnp.zeros_like(acc)

        def run(g, carry, first=first):
            items = [packed[first + g * GROUP + u] for u in range(GROUP)]
            sums = []
            for item in items:
                k, s = lax.shift_right_logical(item, 16), lax.shift_right_logical(item, 6) & 1023
                sums.append(jnp.dot(weights[k], pool[s], preferred_element_type=jnp.float32))
            for item, value in zip(items, sums):
                acc[item & 63] += value
            return carry

        lax.fori_loop(0, rounds, run, 0)

        if group == HALF:
            outs[0][...] = acc[1 : 1 + CAP_T]
            continue
        for r in range(2):

            def encode(b, exponents, r=r, out=outs[r]):
                value = acc[1 + r * CAP_T + b]
                most = jnp.max(jnp.abs(value), axis=0, keepdims=True)
                exponent = jnp.ceil(jnp.log(jnp.maximum(most, 1e-37)) * 1.4426950408889634)
                exponent = jnp.maximum(exponent, LOW_EXPONENT)
                scaled = jnp.floor(value * jnp.exp2(15.0 - exponent) + 0.5)
                scaled = jnp.clip(scaled, -32767.0, 32767.0)
                out[pl.ds(pl.multiple_of(b * TILE, TILE), TILE), :] = scaled.astype(jnp.int32).astype(jnp.int16)
                return jnp.where(rows == b, exponent.astype(jnp.int32), exponents)

            exponents = lax.fori_loop(0, CAP_T, encode, jnp.zeros((CAP_T, TILE), jnp.int32))
            outs[r][CAP_T * TILE :, :] = exponents.astype(jnp.int16)
        outs = outs[2:]


def products_call(groups, rare, held, bounds, packed, weights, pool):
    tile = pool.shape[1:]
    smem = pl.BlockSpec(memory_space=pltpu.SMEM)
    vmem = pl.BlockSpec(memory_space=pltpu.VMEM)
    out_shape = []
    for group in groups:
        if group == HALF:
            out_shape += [jax.ShapeDtypeStruct((CAP_T,) + tile, jnp.float32)]
        else:
            out_shape += [jax.ShapeDtypeStruct((CAP_T * tile[0] + CAP_T, tile[1]), jnp.int16)] * 2
    share = held * len(groups) // 3
    return pl.pallas_call(
        functools.partial(products_kernel, groups),
        out_shape=out_shape,
        in_specs=[smem, smem, vmem, vmem],
        out_specs=[vmem] * len(out_shape),
        scratch_shapes=[pltpu.VMEM((1 + 2 * CAP_T,) + tile, jnp.float32)],
        cost_estimate=pl.CostEstimate(
            flops=share * 2 * 128**3, bytes_accessed=8 * 2**20, transcendentals=0
        ),
        compiler_params=pltpu.CompilerParams(vmem_limit_bytes=(48 if rare else 24) * 2**20),
    )(bounds, packed, weights, pool)


def final_kernel(targets, *refs):
    boxes, out, acc, scales = refs[:SPAN], refs[SPAN], refs[SPAN + 1], refs[SPAN + 2]
    acc[...] = jnp.zeros_like(acc)
    for s in range(SPAN):
        if s != HALF:
            scales[s] = jnp.exp2(boxes[s][CAP_T * TILE :, :].astype(jnp.float32) - 15.0)

    def one(b, carry):
        for s in range(SPAN):
            if s == HALF:
                value = boxes[s][b]
            else:
                rows = pl.ds(pl.multiple_of(b * TILE, TILE), TILE)
                value = boxes[s][rows, :].astype(jnp.float32) * scales[s, pl.ds(b, 1), :]
            acc[targets[s * CAP_T + b]] += value
        return carry

    lax.fori_loop(0, CAP_T, one, 0)

    def close(g, carry):
        for u in range(GROUP):
            out[g * GROUP + u] = acc[1 + g * GROUP + u].astype(out.dtype)
        return carry

    lax.fori_loop(0, TB_DEV // GROUP, close, 0)


def final_call(targets, boxes):
    tile = boxes[HALF].shape[1:]
    vmem = pl.BlockSpec(memory_space=pltpu.VMEM)
    return pl.pallas_call(
        final_kernel,
        out_shape=jax.ShapeDtypeStruct((TB_DEV,) + tile, jnp.bfloat16),
        in_specs=[pl.BlockSpec(memory_space=pltpu.SMEM)] + [vmem] * SPAN,
        out_specs=vmem,
        scratch_shapes=[
            pltpu.VMEM((1 + TB_DEV,) + tile, jnp.float32),
            pltpu.VMEM((SPAN, CAP_T, tile[1]), jnp.float32),
        ],
        name="final_sum",
        compiler_params=pltpu.CompilerParams(vmem_limit_bytes=16 * 2**20),
    )(targets, *boxes)


def named_blocks(ids, first, nb):
    rel = ids - (first - HALF) * nb
    high, low = rel // nb, rel % nb
    high = high[:, None, :] == jnp.arange(SPAN, dtype=jnp.int32)[None, :, None]
    low = low[:, :, None] == jnp.arange(nb, dtype=jnp.int32)[None, None, :]
    counts = lax.dot_general(
        high.astype(jnp.bfloat16),
        low.astype(jnp.bfloat16),
        (((2,), (1,)), ((0,), (0,))),
        preferred_element_type=jnp.float32,
    )
    return counts > 0.5


def wanted(every, role):
    owners = every.shape[0] - 2 * HALF

    def asked_from(step):
        return every[HALF + step : HALF + step + owners, HALF - step]

    role = role[:, None]
    before, after = asked_from(-1), asked_from(1)
    even = role % 2 == 0
    union = asked_from(-2) | asked_from(2) | (even & before) | (~even & after)
    edge = ((role == 0) & before) | ((role == 3) & after)
    beside = (even & after) | (~even & before)
    return union, edge, beside


def body(source_field, weight_blocks, source_ids, target_ids):
    devices = lax.axis_size(AXES)
    n_gy = lax.axis_size("gy")
    me = lax.axis_index(AXES)
    held = weight_blocks.shape[0]
    nb = source_field.shape[0]
    blocks = jnp.arange(nb, dtype=jnp.int32)
    span = 2 * HALF
    ids = jnp.pad(source_ids.reshape(devices, held), ((span, span), (0, 0)), constant_values=-(2**20))
    window = lax.dynamic_slice_in_dim(ids, me, 2 * span + 1, 0)
    sender = me - span + jnp.arange(2 * span + 1, dtype=jnp.int32)[:, None]
    role = (me - HALF + QUAD + jnp.arange(SPAN, dtype=jnp.int32)) % QUAD
    union, edge, beside = wanted(named_blocks(window, sender, nb), role)
    rest = union & ~edge
    sets = jnp.stack([edge, rest, beside]).astype(jnp.bfloat16)
    earlier = (blocks[:, None] < blocks[None, :]).astype(jnp.bfloat16)
    ranks = jnp.einsum("sdb,bc->sdc", sets, earlier, preferred_element_type=jnp.float32).astype(jnp.int32)
    sizes = jnp.sum(sets.astype(jnp.float32), axis=2, keepdims=True).astype(jnp.int32)
    order = jnp.where(
        edge,
        ranks[0],
        jnp.where(rest, sizes[0] + ranks[1], sizes[0] + sizes[1] + blocks[None, :] - ranks[0] - ranks[1]),
    )
    aside = jnp.where(beside, ranks[2], nb)

    r = me % QUAD
    partner = HALF + 1 - 2 * (r % 2)
    mine = jnp.concatenate([aside[HALF : HALF + 1], order[HALF : HALF + 1]])
    chosen = jnp.sum(
        jnp.where(mine[:, None, :] == blocks[None, :, None], blocks[None, None, :], 0), axis=2
    )
    sel = jnp.concatenate([chosen[0, :CAP_S], chosen[1]])

    base_a, base_b, base_c, base_h, base_o = 0, nb, 2 * nb, 3 * nb, 3 * nb + CAP_S
    regions = jnp.array(
        [
            [base_b, base_c, base_o, base_h, base_a],
            [base_c, base_h, base_o, base_a, base_b],
            [base_b, base_a, base_o, base_h, base_c],
            [base_a, base_h, base_o, base_c, base_b],
        ],
        jnp.int32,
    )
    region = lax.dynamic_slice_in_dim(regions, r, 1, 0).reshape(SPAN, 1)
    from_partner = lax.dynamic_slice_in_dim(aside, partner, 1, 0)
    table = jnp.where(
        region == base_o, blocks[None, :], jnp.where(region == base_h, from_partner, order)
    )
    table = (region + table).reshape(-1)
    own_src = rows_of(source_ids, me, devices, held)
    low = (me - HALF) * nb
    hits = (own_src - low)[:, None] == jnp.arange(SPAN * nb, dtype=jnp.int32)[None, :]
    place = jnp.sum(jnp.where(hits, table[None, :], 0), axis=1)

    own_tgt = rows_of(target_ids, me, devices, held)
    low = (me - HALF) * TB_DEV
    tgt_asked = named(own_tgt, low, SPAN * TB_DEV).reshape(SPAN, TB_DEV)
    steps = jnp.arange(SPAN, dtype=jnp.int32)[:, None] - HALF
    tgt_group = HALF - jnp.abs(steps)
    tgt_slot = 1 + ranks_of(tgt_asked) + jnp.where(steps > 0, CAP_T, 0)
    hits = (own_tgt - low)[:, None] == jnp.arange(SPAN * TB_DEV, dtype=jnp.int32)[None, :]
    marks = jnp.sum(jnp.where(hits, (tgt_slot + 64 * tgt_group).reshape(-1)[None, :], 0), axis=1)
    group, slot = marks // 64, marks % 64

    index = jnp.arange(held, dtype=jnp.int32)
    groups = jnp.arange(4, dtype=jnp.int32)
    sizes = jnp.sum((group[None, :] == groups[:, None]).astype(jnp.int32), axis=1)
    sizes = (sizes + GROUP - 1) // GROUP * GROUP
    bounds = jnp.sum(jnp.where(groups[None, :] < groups[:, None], sizes[None, :], 0), axis=1)
    earlier = (group[:, None] == group[None, :]) & (index[:, None] < index[None, :])
    position = jnp.sum(earlier.astype(jnp.int32), axis=0)
    position = position + jnp.sum(
        jnp.where(group[None, :] == groups[:, None], bounds[:, None], 0), axis=0
    )
    item = (index * 1024 + place) * 64 + slot
    spots = jnp.arange(held + 4 * GROUP, dtype=jnp.int32)
    packed = jnp.sum(jnp.where(position[None, :] == spots[:, None], item[None, :], 0), axis=1)

    box_asked = []
    for step in range(-HALF, HALF + 1):
        sender = me - step
        valid = (sender >= 0) & (sender < devices)
        rows = rows_of(target_ids, sender, devices, held)
        box_asked.append(named(rows, me * TB_DEV, TB_DEV) & valid)
    box_asked = jnp.stack(box_asked)
    spot = jnp.where(box_asked, ranks_of(box_asked), -1)
    targets = jnp.sum(
        jnp.where(
            spot[:, None, :] == jnp.arange(CAP_T, dtype=jnp.int32)[None, :, None],
            1 + jnp.arange(TB_DEV, dtype=jnp.int32)[None, None, :],
            0,
        ),
        axis=2,
    ).reshape(-1)

    def finish(rare, bounds, packed, sel, targets, source_field, weight_blocks, source_ids):
        sel, bounds, packed, targets = lax.optimization_barrier((sel, bounds, packed, targets))
        pool = exchange_call(n_gy, devices, rare, sel, source_field)
        weights = weight_blocks
        boxes = [None] * SPAN
        below, above = products_call((0,), rare, held, bounds, packed, weights, pool)
        bounds, below, above = lax.optimization_barrier((bounds, below, above))
        boxes[0] = passed_along(below, -2)
        boxes[4] = passed_along(above, 2)
        below, above, own = products_call((1, 2), rare, held, bounds, packed, weights, pool)
        boxes[1] = passed_along(below, -1)
        boxes[3] = passed_along(above, 1)
        boxes[2], source_ids = lax.optimization_barrier((own, source_ids))
        return final_call(targets, boxes), source_ids

    arrays = (bounds, packed, sel, targets, source_field, weight_blocks, source_ids)
    result, late_ids = finish(False, *arrays)
    every = named_blocks(
        late_ids.reshape(devices, held), jnp.arange(devices, dtype=jnp.int32)[:, None], nb
    )
    every = jnp.pad(every, ((HALF, HALF), (0, 0), (0, 0)))
    union, _, _ = wanted(every, jnp.arange(devices, dtype=jnp.int32) % QUAD)
    most = jnp.max(jnp.sum(union.astype(jnp.int32), axis=1))
    return lax.cond(
        most > nb - RARE, lambda result, *arrays: finish(True, *arrays)[0], lambda result, *arrays: result, result, *arrays
    )


def solution(mesh):
    return jax.shard_map(
        body,
        mesh=mesh,
        in_specs=(P(AXES, None, None), P(AXES, None, None), P(), P()),
        out_specs=P(AXES, None, None),
        check_vma=False,
    )
```

```python
import functools

import jax
import jax.numpy as jnp
from jax import lax
from jax.experimental import pallas as pl
from jax.experimental.pallas import tpu as pltpu
from jax.sharding import PartitionSpec as P


HALF = 2
TB_DEV = 64
CAP_S = 64
CAP_T = 16
SPAN = 2 * HALF + 1
AXES = ("gx", "gy")
MESH = pl.DeviceIdType.MESH
QUAD = 4
CHUNK = 4
GROUP = 32
TILE = 128
RARE = 12
LOW_EXPONENT = -110.0


def passed_along(value, steps):
    count = lax.axis_size(AXES)
    initial, last = (max(0, -steps), min(count, count - steps))
    return lax.ppermute(value, AXES, [(source, source + steps) for source in range(initial, last)])


def rows_of(ids, device, devices, held):
    clamped = jnp.clip(device, 0, devices - 1)
    return lax.dynamic_slice_in_dim(ids, clamped * held, held, 0)


def named(rows, low, count):
    return jnp.any(rows[:, None] == low + jnp.arange(count, dtype=jnp.int32)[None, :], axis=0)


def ranks_of(asked):
    count = asked.shape[1]
    before = jnp.arange(count)[:, None] < jnp.arange(count)[None, :]
    return jnp.sum((asked[:, :, None] & before[None]).astype(jnp.int32), axis=1)


def exchange_kernel(devices, n_gy, count, sel, src, recv, srcv, hst, xst, lsem, rsem, ssem):
    nb = src.shape[0]
    pieces = count // CHUNK
    half = CAP_S // CHUNK
    me = lax.axis_index("gx") * n_gy + lax.axis_index("gy")
    r = lax.rem(me, QUAD)
    inner = (r == 1) | (r == 2)
    outer = jnp.logical_not(inner)
    sgn = jnp.where(r < 2, 1, -1)
    partner = me + 1 - 2 * lax.rem(r, 2)
    near = me + sgn
    far = me + 2 * sgn
    to = me + QUAD * sgn
    source = me - QUAD * sgn
    has_to = (to >= 0) & (to < devices)
    has_from = (source >= 0) & (source < devices)
    base_a, base_b, base_c, base_h, base_o = 0, nb, 2 * nb, 3 * nb, 3 * nb + CAP_S

    def at(device):
        return (device // n_gy, lax.rem(device, n_gy))

    barrier = pltpu.get_barrier_semaphore()

    def greet(device):
        pl.semaphore_signal(barrier, inc=1, device_id=at(device), device_id_type=MESH)

    greet(partner)
    greet(far)
    pl.when(inner)(lambda: greet(near))
    pl.when(has_to)(lambda: greet(to))
    pl.when(has_from)(lambda: greet(source))
    peers = 2 + inner.astype(jnp.int32) + has_to.astype(jnp.int32) + has_from.astype(jnp.int32)
    pl.semaphore_wait(barrier, peers)

    def piece(base, k):
        return recv.at[pl.ds(base + k * CHUNK, CHUNK)]

    def copy(ref, base, k, send, got, device):
        return pltpu.make_async_remote_copy(
            src_ref=ref,
            dst_ref=piece(base, k),
            send_sem=ssem.at[send, k],
            recv_sem=rsem.at[got, k],
            device_id=at(device),
            device_id_type=MESH,
        )

    def cross_inner(k):
        return copy(xst.at[pl.ds(k * CHUNK, CHUNK)], base_a, k, 0, 0, near)

    def cross_outer(k):
        return copy(xst.at[pl.ds(k * CHUNK, CHUNK)], base_b, k, 0, 1, far)

    def side(k):
        return copy(hst.at[pl.ds(k * CHUNK, CHUNK)], base_h, k, 1, 3, partner)

    def ahead(k):
        return copy(piece(base_a, k), base_a, k, 2, 0, partner)

    def over_outer(k):
        return copy(piece(base_a, k), base_b, k, 3, 1, to)

    def over_inner(k):
        return copy(piece(base_b, k), base_c, k, 3, 2, to)

    def last(k):
        return copy(piece(base_c, k), base_c, k, 4, 2, partner)

    def await_piece(base, got, k):
        copy(piece(base, k), base, k, 0, got, partner).wait_recv()

    load = pltpu.make_async_copy(src, srcv, lsem.at[0])
    load.start()
    keep = pltpu.make_async_copy(src, recv.at[pl.ds(base_o, nb)], lsem.at[1])
    load.wait()

    def pick(j, carry):
        for u in range(CHUNK):
            xst[j * CHUNK + u] = srcv[sel[CAP_S + j * CHUNK + u]]
        return carry

    def pick_side(j, carry):
        for u in range(CHUNK):
            hst[j * CHUNK + u] = srcv[sel[j * CHUNK + u]]
        return carry

    lax.fori_loop(0, pieces, pick, 0)
    lax.fori_loop(0, half, pick_side, 0)

    @pl.when(inner)
    def _():
        for k in range(pieces):
            cross_inner(k).start()
        for k in range(half):
            side(k).start()

    keep.start()

    @pl.when(outer)
    def _():
        for k in range(pieces):
            cross_outer(k).start()
        for k in range(half):
            side(k).start()
        for k in range(pieces):
            await_piece(base_a, 0, k)

            @pl.when(has_to)
            def _():
                over_outer(k).start()

        @pl.when(has_from)
        def _():
            for k in range(pieces):
                await_piece(base_b, 1, k)
            for k in range(half):
                await_piece(base_c, 2, k)

        for k in range(pieces):
            cross_outer(k).wait_send()

        @pl.when(has_to)
        def _():
            for k in range(pieces):
                over_outer(k).wait_send()

    @pl.when(inner)
    def _():
        def from_far(k):
            await_piece(base_b, 1, k)

            @pl.when(has_to)
            def _():
                over_inner(k).start()

        def from_shift(k):
            if 0 <= k < half:

                @pl.when(has_from)
                def _():
                    await_piece(base_c, 2, k)
                    last(k).start()

        for k in range(pieces):
            from_far(k)
            from_shift(k - 1)
        for k in range(pieces):
            await_piece(base_a, 0, k)
            ahead(k).start()

        @pl.when(has_from)
        def _():
            for k in range(half, pieces):
                await_piece(base_c, 2, k)
            for k in range(half):
                last(k).wait_send()

        for k in range(pieces):
            cross_inner(k).wait_send()
            ahead(k).wait_send()

        @pl.when(has_to)
        def _():
            for k in range(pieces):
                over_inner(k).wait_send()

    for k in range(half):
        await_piece(base_h, 3, k)
        side(k).wait_send()
    keep.wait()


def exchange_call(n_gy, devices, rare, sel, source_field):
    nb = source_field.shape[0]
    tile = source_field.shape[1:]
    kind = source_field.dtype
    count = nb if rare else nb - RARE
    pieces = count // CHUNK
    anywhere = pl.BlockSpec(memory_space=pl.ANY)
    vmem = pl.BlockSpec(memory_space=pltpu.VMEM)
    return pl.pallas_call(
        functools.partial(exchange_kernel, devices, n_gy, count),
        out_shape=jax.ShapeDtypeStruct((4 * nb + CAP_S,) + tile, kind),
        in_specs=[pl.BlockSpec(memory_space=pltpu.SMEM), anywhere],
        out_specs=anywhere if rare else vmem,
        scratch_shapes=[
            pltpu.VMEM((nb,) + tile, kind),
            pltpu.VMEM((CAP_S,) + tile, kind),
            pltpu.VMEM((count,) + tile, kind),
            pltpu.SemaphoreType.DMA((3,)),
            pltpu.SemaphoreType.DMA((4, pieces)),
            pltpu.SemaphoreType.DMA((5, pieces)),
        ],
        name="exchange_all" if rare else "exchange",
        cost_estimate=pl.CostEstimate(flops=2 * 10**10, bytes_accessed=8 * 2**20, transcendentals=0),
        compiler_params=pltpu.CompilerParams(
            collective_id=int(rare), has_side_effects=True, vmem_limit_bytes=12 * 2**20
        ),
    )(sel, source_field)


def products_kernel(groups, bounds, packed, weights, pool, *refs):
    outs, acc = refs[:-1], refs[-1]
    rows = lax.broadcasted_iota(jnp.int32, (CAP_T, TILE), 0)
    for group in groups:
        first = bounds[group]
        rounds = (bounds[group + 1] - first) // GROUP
        acc[...] = jnp.zeros_like(acc)

        def run(g, carry, first=first):
            items = [packed[first + g * GROUP + u] for u in range(GROUP)]
            sums = []
            for item in items:
                k, s = lax.shift_right_logical(item, 16), lax.shift_right_logical(item, 6) & 1023
                sums.append(jnp.dot(weights[k], pool[s], preferred_element_type=jnp.float32))
            for item, value in zip(items, sums):
                acc[item & 63] += value
            return carry

        lax.fori_loop(0, rounds, run, 0)

        if group == HALF:
            outs[0][...] = acc[1 : 1 + CAP_T]
            continue
        for r in range(2):

            def encode(b, exponents, r=r, out=outs[r]):
                value = acc[1 + r * CAP_T + b]
                most = jnp.max(jnp.abs(value), axis=0, keepdims=True)
                exponent = jnp.ceil(jnp.log(jnp.maximum(most, 1e-37)) * 1.4426950408889634)
                exponent = jnp.maximum(exponent, LOW_EXPONENT)
                scaled = jnp.floor(value * jnp.exp2(15.0 - exponent) + 0.5)
                scaled = jnp.clip(scaled, -32767.0, 32767.0)
                out[pl.ds(pl.multiple_of(b * TILE, TILE), TILE), :] = scaled.astype(jnp.int32).astype(jnp.int16)
                return jnp.where(rows == b, exponent.astype(jnp.int32), exponents)

            exponents = lax.fori_loop(0, CAP_T, encode, jnp.zeros((CAP_T, TILE), jnp.int32))
            outs[r][CAP_T * TILE :, :] = exponents.astype(jnp.int16)
        outs = outs[2:]


def products_call(groups, rare, held, bounds, packed, weights, pool):
    tile = pool.shape[1:]
    smem = pl.BlockSpec(memory_space=pltpu.SMEM)
    vmem = pl.BlockSpec(memory_space=pltpu.VMEM)
    out_shape = []
    for group in groups:
        if group == HALF:
            out_shape += [jax.ShapeDtypeStruct((CAP_T,) + tile, jnp.float32)]
        else:
            out_shape += [jax.ShapeDtypeStruct((CAP_T * tile[0] + CAP_T, tile[1]), jnp.int16)] * 2
    share = held * len(groups) // 3
    return pl.pallas_call(
        functools.partial(products_kernel, groups),
        out_shape=out_shape,
        in_specs=[smem, smem, vmem, vmem],
        out_specs=[vmem] * len(out_shape),
        scratch_shapes=[pltpu.VMEM((1 + 2 * CAP_T,) + tile, jnp.float32)],
        cost_estimate=pl.CostEstimate(
            flops=share * 2 * 128**3, bytes_accessed=8 * 2**20, transcendentals=0
        ),
        compiler_params=pltpu.CompilerParams(vmem_limit_bytes=(48 if rare else 24) * 2**20),
    )(bounds, packed, weights, pool)


def final_kernel(targets, *refs):
    boxes, out, acc, scales = refs[:SPAN], refs[SPAN], refs[SPAN + 1], refs[SPAN + 2]
    acc[...] = jnp.zeros_like(acc)
    for s in range(SPAN):
        if s != HALF:
            scales[s] = jnp.exp2(boxes[s][CAP_T * TILE :, :].astype(jnp.float32) - 15.0)

    def one(b, carry):
        for s in range(SPAN):
            if s == HALF:
                value = boxes[s][b]
            else:
                rows = pl.ds(pl.multiple_of(b * TILE, TILE), TILE)
                value = boxes[s][rows, :].astype(jnp.float32) * scales[s, pl.ds(b, 1), :]
            acc[targets[s * CAP_T + b]] += value
        return carry

    lax.fori_loop(0, CAP_T, one, 0)

    def close(g, carry):
        for u in range(GROUP):
            out[g * GROUP + u] = acc[1 + g * GROUP + u].astype(out.dtype)
        return carry

    lax.fori_loop(0, TB_DEV // GROUP, close, 0)


def final_call(targets, boxes):
    tile = boxes[HALF].shape[1:]
    vmem = pl.BlockSpec(memory_space=pltpu.VMEM)
    return pl.pallas_call(
        final_kernel,
        out_shape=jax.ShapeDtypeStruct((TB_DEV,) + tile, jnp.bfloat16),
        in_specs=[pl.BlockSpec(memory_space=pltpu.SMEM)] + [vmem] * SPAN,
        out_specs=vmem,
        scratch_shapes=[
            pltpu.VMEM((1 + TB_DEV,) + tile, jnp.float32),
            pltpu.VMEM((SPAN, CAP_T, tile[1]), jnp.float32),
        ],
        name="final_sum",
        compiler_params=pltpu.CompilerParams(vmem_limit_bytes=16 * 2**20),
    )(targets, *boxes)


def named_blocks(ids, first, nb):
    rel = ids - (first - HALF) * nb
    high, low = rel // nb, rel % nb
    high = high[:, None, :] == jnp.arange(SPAN, dtype=jnp.int32)[None, :, None]
    low = low[:, :, None] == jnp.arange(nb, dtype=jnp.int32)[None, None, :]
    counts = lax.dot_general(
        high.astype(jnp.bfloat16),
        low.astype(jnp.bfloat16),
        (((2,), (1,)), ((0,), (0,))),
        preferred_element_type=jnp.float32,
    )
    return counts > 0.5


def wanted(every, role):
    owners = every.shape[0] - 2 * HALF

    def asked_from(step):
        return every[HALF + step : HALF + step + owners, HALF - step]

    role = role[:, None]
    before, after = asked_from(-1), asked_from(1)
    even = (role & 1) == 0
    union = asked_from(-2) | asked_from(2) | (even & before) | (~even & after)
    edge = ((role == 0) & before) | ((role == 3) & after)
    beside = (even & after) | (~even & before)
    return union, edge, beside


def body(source_field, weight_blocks, source_ids, target_ids):
    devices = lax.axis_size(AXES)
    n_gy = lax.axis_size("gy")
    me = lax.axis_index(AXES)
    held = weight_blocks.shape[0]
    nb = source_field.shape[0]
    blocks = jnp.arange(nb, dtype=jnp.int32)
    span = 2 * HALF
    ids = jnp.pad(source_ids, (span * held, span * held), constant_values=-(2**20))
    window = lax.dynamic_slice_in_dim(ids, me * held, (2 * span + 1) * held, 0)
    window = window.reshape(2 * span + 1, held)
    sender = me - span + jnp.arange(2 * span + 1, dtype=jnp.int32)[:, None]
    role = (me - HALF + jnp.arange(SPAN, dtype=jnp.int32)) & (QUAD - 1)
    union, edge, beside = wanted(named_blocks(window, sender, nb), role)
    rest = union & ~edge
    sets = jnp.stack([edge, rest, beside]).astype(jnp.bfloat16)
    earlier = (blocks[:, None] < blocks[None, :]).astype(jnp.bfloat16)
    ranks = jnp.einsum("sdb,bc->sdc", sets, earlier, preferred_element_type=jnp.float32).astype(jnp.int32)
    sizes = jnp.sum(sets.astype(jnp.float32), axis=2, keepdims=True).astype(jnp.int32)
    order = jnp.where(
        edge,
        ranks[0],
        jnp.where(rest, sizes[0] + ranks[1], sizes[0] + sizes[1] + blocks[None, :] - ranks[0] - ranks[1]),
    )
    aside = jnp.where(beside, ranks[2], nb)

    r = me & (QUAD - 1)
    partner = HALF + 1 - 2 * (r & 1)
    mine = jnp.concatenate([aside[HALF : HALF + 1], order[HALF : HALF + 1]])
    chosen = jnp.sum(
        jnp.where(mine[:, None, :] == blocks[None, :, None], blocks[None, None, :], 0), axis=2
    )
    sel = jnp.concatenate([chosen[0, :CAP_S], chosen[1]])

    base_a, base_b, base_c, base_h, base_o = 0, nb, 2 * nb, 3 * nb, 3 * nb + CAP_S
    regions = jnp.array(
        [
            [base_b, base_c, base_o, base_h, base_a],
            [base_c, base_h, base_o, base_a, base_b],
            [base_b, base_a, base_o, base_h, base_c],
            [base_a, base_h, base_o, base_c, base_b],
        ],
        jnp.int32,
    )
    region = lax.dynamic_slice_in_dim(regions, r, 1, 0).reshape(SPAN, 1)
    from_partner = lax.dynamic_slice_in_dim(aside, partner, 1, 0)
    table = jnp.where(
        region == base_o, blocks[None, :], jnp.where(region == base_h, from_partner, order)
    )
    table = (region + table).reshape(-1)
    own_src = rows_of(source_ids, me, devices, held)
    low = (me - HALF) * nb
    hits = (own_src - low)[:, None] == jnp.arange(SPAN * nb, dtype=jnp.int32)[None, :]
    place = jnp.sum(jnp.where(hits, table[None, :], 0), axis=1)

    own_tgt = rows_of(target_ids, me, devices, held)
    low = (me - HALF) * TB_DEV
    tgt_asked = named(own_tgt, low, SPAN * TB_DEV).reshape(SPAN, TB_DEV)
    steps = jnp.arange(SPAN, dtype=jnp.int32)[:, None] - HALF
    tgt_group = HALF - jnp.abs(steps)
    tgt_slot = 1 + ranks_of(tgt_asked) + jnp.where(steps > 0, CAP_T, 0)
    hits = (own_tgt - low)[:, None] == jnp.arange(SPAN * TB_DEV, dtype=jnp.int32)[None, :]
    marks = jnp.sum(jnp.where(hits, (tgt_slot + 64 * tgt_group).reshape(-1)[None, :], 0), axis=1)
    group, slot = marks // 64, marks % 64

    index = jnp.arange(held, dtype=jnp.int32)
    groups = jnp.arange(4, dtype=jnp.int32)
    sizes = jnp.sum((group[None, :] == groups[:, None]).astype(jnp.int32), axis=1)
    sizes = (sizes + GROUP - 1) // GROUP * GROUP
    bounds = jnp.sum(jnp.where(groups[None, :] < groups[:, None], sizes[None, :], 0), axis=1)
    earlier = (group[:, None] == group[None, :]) & (index[:, None] < index[None, :])
    position = jnp.sum(earlier.astype(jnp.int32), axis=0)
    position = position + jnp.sum(
        jnp.where(group[None, :] == groups[:, None], bounds[:, None], 0), axis=0
    )
    item = (index * 1024 + place) * 64 + slot
    spots = jnp.arange(held + 4 * GROUP, dtype=jnp.int32)
    packed = jnp.sum(jnp.where(position[None, :] == spots[:, None], item[None, :], 0), axis=1)

    box_asked = []
    for step in range(-HALF, HALF + 1):
        sender = me - step
        valid = (sender >= 0) & (sender < devices)
        rows = rows_of(target_ids, sender, devices, held)
        box_asked.append(named(rows, me * TB_DEV, TB_DEV) & valid)
    box_asked = jnp.stack(box_asked)
    spot = jnp.where(box_asked, ranks_of(box_asked), -1)
    targets = jnp.sum(
        jnp.where(
            spot[:, None, :] == jnp.arange(CAP_T, dtype=jnp.int32)[None, :, None],
            1 + jnp.arange(TB_DEV, dtype=jnp.int32)[None, None, :],
            0,
        ),
        axis=2,
    ).reshape(-1)

    def finish(rare, bounds, packed, sel, targets, source_field, weight_blocks, source_ids):
        sel, bounds, packed, targets = lax.optimization_barrier((sel, bounds, packed, targets))
        pool = exchange_call(n_gy, devices, rare, sel, source_field)
        weights = weight_blocks
        boxes = [None] * SPAN
        below, above = products_call((0,), rare, held, bounds, packed, weights, pool)
        bounds, below, above = lax.optimization_barrier((bounds, below, above))
        boxes[0] = passed_along(below, -2)
        boxes[4] = passed_along(above, 2)
        below, above, own = products_call((1, 2), rare, held, bounds, packed, weights, pool)
        boxes[1] = passed_along(below, -1)
        boxes[3] = passed_along(above, 1)
        boxes[2], source_ids = lax.optimization_barrier((own, source_ids))
        return final_call(targets, boxes), source_ids

    arrays = (bounds, packed, sel, targets, source_field, weight_blocks, source_ids)
    result, late_ids = finish(False, *arrays)
    every = named_blocks(
        late_ids.reshape(devices, held), jnp.arange(devices, dtype=jnp.int32)[:, None], nb
    )
    every = jnp.pad(every, ((HALF, HALF), (0, 0), (0, 0)))
    union, _, _ = wanted(every, jnp.arange(devices, dtype=jnp.int32) % QUAD)
    most = jnp.max(jnp.sum(union.astype(jnp.int32), axis=1))
    return lax.cond(
        most > nb - RARE, lambda result, *arrays: finish(True, *arrays)[0], lambda result, *arrays: result, result, *arrays
    )


def solution(mesh):
    return jax.shard_map(
        body,
        mesh=mesh,
        in_specs=(P(AXES, None, None), P(AXES, None, None), P(), P()),
        out_specs=P(AXES, None, None),
        check_vma=False,
    )
```

```python
import functools

import jax
import jax.numpy as jnp
from jax import lax
from jax.experimental import pallas as pl
from jax.experimental.pallas import tpu as pltpu
from jax.sharding import PartitionSpec as P


HALF = 2
TB_DEV = 64
CAP_S = 64
CAP_T = 16
SPAN = 2 * HALF + 1
AXES = ("gx", "gy")
MESH = pl.DeviceIdType.MESH
QUAD = 4
CHUNK = 4
GROUP = 32
CLOSE = 8
TILE = 128
RARE = 12
LOW_EXPONENT = -110.0


def passed_along(value, steps):
    count = lax.axis_size(AXES)
    initial, last = (max(0, -steps), min(count, count - steps))
    return lax.ppermute(value, AXES, [(source, source + steps) for source in range(initial, last)])


def rows_of(ids, device, devices, held):
    clamped = jnp.clip(device, 0, devices - 1)
    return lax.dynamic_slice_in_dim(ids, clamped * held, held, 0)


def named(rows, low, count):
    return jnp.any(rows[:, None] == low + jnp.arange(count, dtype=jnp.int32)[None, :], axis=0)


def ranks_of(asked):
    count = asked.shape[1]
    before = jnp.arange(count)[:, None] < jnp.arange(count)[None, :]
    return jnp.sum((asked[:, :, None] & before[None]).astype(jnp.int32), axis=1)


def exchange_kernel(devices, n_gy, count, sel, src, recv, srcv, hst, xst, lsem, rsem, ssem):
    nb = src.shape[0]
    pieces = count // CHUNK
    half = CAP_S // CHUNK
    me = lax.axis_index("gx") * n_gy + lax.axis_index("gy")
    r = lax.rem(me, QUAD)
    inner = (r == 1) | (r == 2)
    outer = jnp.logical_not(inner)
    sgn = jnp.where(r < 2, 1, -1)
    partner = me + 1 - 2 * lax.rem(r, 2)
    near = me + sgn
    far = me + 2 * sgn
    to = me + QUAD * sgn
    source = me - QUAD * sgn
    has_to = (to >= 0) & (to < devices)
    has_from = (source >= 0) & (source < devices)
    base_a, base_b, base_c, base_h, base_o = 0, nb, 2 * nb, 3 * nb, 3 * nb + CAP_S

    def at(device):
        return (device // n_gy, lax.rem(device, n_gy))

    barrier = pltpu.get_barrier_semaphore()

    def greet(device):
        pl.semaphore_signal(barrier, inc=1, device_id=at(device), device_id_type=MESH)

    greet(partner)
    greet(far)
    pl.when(inner)(lambda: greet(near))
    pl.when(has_to)(lambda: greet(to))
    pl.when(has_from)(lambda: greet(source))

    def piece(base, k):
        return recv.at[pl.ds(base + k * CHUNK, CHUNK)]

    def copy(ref, base, k, send, got, device):
        return pltpu.make_async_remote_copy(
            src_ref=ref,
            dst_ref=piece(base, k),
            send_sem=ssem.at[send, k],
            recv_sem=rsem.at[got, k],
            device_id=at(device),
            device_id_type=MESH,
        )

    def cross_inner(k):
        return copy(xst.at[pl.ds(k * CHUNK, CHUNK)], base_a, k, 0, 0, near)

    def cross_outer(k):
        return copy(xst.at[pl.ds(k * CHUNK, CHUNK)], base_b, k, 0, 1, far)

    def side(k):
        return copy(hst.at[pl.ds(k * CHUNK, CHUNK)], base_h, k, 1, 3, partner)

    def ahead(k):
        return copy(piece(base_a, k), base_a, k, 2, 0, partner)

    def over_outer(k):
        return copy(piece(base_a, k), base_b, k, 3, 1, to)

    def over_inner(k):
        return copy(piece(base_b, k), base_c, k, 3, 2, to)

    def last(k):
        return copy(piece(base_c, k), base_c, k, 4, 2, partner)

    def await_piece(base, got, k):
        copy(piece(base, k), base, k, 0, got, partner).wait_recv()

    load = pltpu.make_async_copy(src, srcv, lsem.at[0])
    load.start()
    keep = pltpu.make_async_copy(src, recv.at[pl.ds(base_o, nb)], lsem.at[1])
    load.wait()

    def pick(j, carry):
        for u in range(CHUNK):
            xst[j * CHUNK + u] = srcv[sel[CAP_S + j * CHUNK + u]]
        return carry

    def pick_side(j, carry):
        for u in range(CHUNK):
            hst[j * CHUNK + u] = srcv[sel[j * CHUNK + u]]
        return carry

    lax.fori_loop(0, pieces, pick, 0)
    lax.fori_loop(0, half, pick_side, 0)

    peers = 2 + inner.astype(jnp.int32) + has_to.astype(jnp.int32) + has_from.astype(jnp.int32)
    pl.semaphore_wait(barrier, peers)

    @pl.when(inner)
    def _():
        for k in range(pieces):
            cross_inner(k).start()
        for k in range(half):
            side(k).start()

    keep.start()

    @pl.when(outer)
    def _():
        for k in range(pieces):
            cross_outer(k).start()
        for k in range(half):
            side(k).start()
        for k in range(pieces):
            await_piece(base_a, 0, k)

            @pl.when(has_to)
            def _():
                over_outer(k).start()

        @pl.when(has_from)
        def _():
            for k in range(pieces):
                await_piece(base_b, 1, k)
            for k in range(half):
                await_piece(base_c, 2, k)

        for k in range(pieces):
            cross_outer(k).wait_send()

        @pl.when(has_to)
        def _():
            for k in range(pieces):
                over_outer(k).wait_send()

    @pl.when(inner)
    def _():
        def from_far(k):
            await_piece(base_b, 1, k)

            @pl.when(has_to)
            def _():
                over_inner(k).start()

        def from_shift(k):
            if 0 <= k < half:

                @pl.when(has_from)
                def _():
                    await_piece(base_c, 2, k)
                    last(k).start()

        for k in range(pieces):
            from_far(k)
            from_shift(k - 1)
        for k in range(pieces):
            await_piece(base_a, 0, k)
            ahead(k).start()

        @pl.when(has_from)
        def _():
            for k in range(half, pieces):
                await_piece(base_c, 2, k)
            for k in range(half):
                last(k).wait_send()

        for k in range(pieces):
            cross_inner(k).wait_send()
            ahead(k).wait_send()

        @pl.when(has_to)
        def _():
            for k in range(pieces):
                over_inner(k).wait_send()

    for k in range(half):
        await_piece(base_h, 3, k)
        side(k).wait_send()
    keep.wait()


def exchange_call(n_gy, devices, rare, sel, source_field):
    nb = source_field.shape[0]
    tile = source_field.shape[1:]
    kind = source_field.dtype
    count = nb if rare else nb - RARE
    pieces = count // CHUNK
    anywhere = pl.BlockSpec(memory_space=pl.ANY)
    vmem = pl.BlockSpec(memory_space=pltpu.VMEM)
    return pl.pallas_call(
        functools.partial(exchange_kernel, devices, n_gy, count),
        out_shape=jax.ShapeDtypeStruct((4 * nb + CAP_S,) + tile, kind),
        in_specs=[pl.BlockSpec(memory_space=pltpu.SMEM), anywhere],
        out_specs=anywhere if rare else vmem,
        scratch_shapes=[
            pltpu.VMEM((nb,) + tile, kind),
            pltpu.VMEM((CAP_S,) + tile, kind),
            pltpu.VMEM((count,) + tile, kind),
            pltpu.SemaphoreType.DMA((3,)),
            pltpu.SemaphoreType.DMA((4, pieces)),
            pltpu.SemaphoreType.DMA((5, pieces)),
        ],
        name="exchange_all" if rare else "exchange",
        cost_estimate=pl.CostEstimate(flops=2 * 10**10, bytes_accessed=8 * 2**20, transcendentals=0),
        compiler_params=pltpu.CompilerParams(
            collective_id=int(rare), has_side_effects=True, vmem_limit_bytes=12 * 2**20
        ),
    )(sel, source_field)


def products_kernel(groups, bounds, packed, weights, pool, *refs):
    outs, acc = refs[:-1], refs[-1]
    rows = lax.broadcasted_iota(jnp.int32, (CAP_T, TILE), 0)
    for group in groups:
        first = bounds[group]
        rounds = (bounds[group + 1] - first) // GROUP
        acc[...] = jnp.zeros_like(acc)

        def run(g, carry, first=first):
            items = [packed[first + g * GROUP + u] for u in range(GROUP)]
            sums = []
            for item in items:
                k, s = lax.shift_right_logical(item, 16), lax.shift_right_logical(item, 6) & 1023
                sums.append(jnp.dot(weights[k], pool[s], preferred_element_type=jnp.float32))
            for item, value in zip(items, sums):
                acc[item & 63] += value
            return carry

        lax.fori_loop(0, rounds, run, 0)

        if group == HALF:
            outs[0][...] = acc[1 : 1 + CAP_T]
            continue
        for r in range(2):

            def encode(b, exponents, r=r, out=outs[r]):
                value = acc[1 + r * CAP_T + b]
                most = jnp.max(jnp.abs(value), axis=0, keepdims=True)
                exponent = jnp.ceil(jnp.log(jnp.maximum(most, 1e-37)) * 1.4426950408889634)
                exponent = jnp.maximum(exponent, LOW_EXPONENT)
                scaled = jnp.floor(value * jnp.exp2(15.0 - exponent) + 0.5)
                scaled = jnp.clip(scaled, -32767.0, 32767.0)
                out[pl.ds(pl.multiple_of(b * TILE, TILE), TILE), :] = scaled.astype(jnp.int32).astype(jnp.int16)
                return jnp.where(rows == b, exponent.astype(jnp.int32), exponents)

            exponents = lax.fori_loop(0, CAP_T, encode, jnp.zeros((CAP_T, TILE), jnp.int32))
            outs[r][CAP_T * TILE :, :] = exponents.astype(jnp.int16)
        outs = outs[2:]


def products_call(groups, rare, held, bounds, packed, weights, pool):
    tile = pool.shape[1:]
    smem = pl.BlockSpec(memory_space=pltpu.SMEM)
    vmem = pl.BlockSpec(memory_space=pltpu.VMEM)
    out_shape = []
    for group in groups:
        if group == HALF:
            out_shape += [jax.ShapeDtypeStruct((CAP_T,) + tile, jnp.float32)]
        else:
            out_shape += [jax.ShapeDtypeStruct((CAP_T * tile[0] + CAP_T, tile[1]), jnp.int16)] * 2
    share = held * len(groups) // 3
    return pl.pallas_call(
        functools.partial(products_kernel, groups),
        out_shape=out_shape,
        in_specs=[smem, smem, vmem, vmem],
        out_specs=[vmem] * len(out_shape),
        scratch_shapes=[pltpu.VMEM((1 + 2 * CAP_T,) + tile, jnp.float32)],
        cost_estimate=pl.CostEstimate(
            flops=share * 2 * 128**3, bytes_accessed=8 * 2**20, transcendentals=0
        ),
        compiler_params=pltpu.CompilerParams(vmem_limit_bytes=(48 if rare else 24) * 2**20),
    )(bounds, packed, weights, pool)


def final_kernel(targets, *refs):
    boxes, out, acc, scales = refs[:SPAN], refs[SPAN], refs[SPAN + 1], refs[SPAN + 2]
    acc[...] = jnp.zeros_like(acc)
    for s in range(SPAN):
        if s != HALF:
            scales[s] = jnp.exp2(boxes[s][CAP_T * TILE :, :].astype(jnp.float32) - 15.0)

    def one(b, carry):
        for s in range(SPAN):
            if s == HALF:
                value = boxes[s][b]
            else:
                rows = pl.ds(pl.multiple_of(b * TILE, TILE), TILE)
                value = boxes[s][rows, :].astype(jnp.float32) * scales[s, pl.ds(b, 1), :]
            acc[targets[s * CAP_T + b]] += value
        return carry

    lax.fori_loop(0, CAP_T, one, 0)

    def close(g, carry):
        for u in range(CLOSE):
            out[g * CLOSE + u] = acc[1 + g * CLOSE + u].astype(out.dtype)
        return carry

    lax.fori_loop(0, TB_DEV // CLOSE, close, 0)


def final_call(targets, boxes):
    tile = boxes[HALF].shape[1:]
    vmem = pl.BlockSpec(memory_space=pltpu.VMEM)
    return pl.pallas_call(
        final_kernel,
        out_shape=jax.ShapeDtypeStruct((TB_DEV,) + tile, jnp.bfloat16),
        in_specs=[pl.BlockSpec(memory_space=pltpu.SMEM)] + [vmem] * SPAN,
        out_specs=vmem,
        scratch_shapes=[
            pltpu.VMEM((1 + TB_DEV,) + tile, jnp.float32),
            pltpu.VMEM((SPAN, CAP_T, tile[1]), jnp.float32),
        ],
        name="final_sum",
        compiler_params=pltpu.CompilerParams(vmem_limit_bytes=16 * 2**20),
    )(targets, *boxes)


def named_blocks(ids, first, nb):
    rel = ids - (first - HALF) * nb
    high, low = rel // nb, rel % nb
    high = high[:, None, :] == jnp.arange(SPAN, dtype=jnp.int32)[None, :, None]
    low = low[:, :, None] == jnp.arange(nb, dtype=jnp.int32)[None, None, :]
    counts = lax.dot_general(
        high.astype(jnp.bfloat16),
        low.astype(jnp.bfloat16),
        (((2,), (1,)), ((0,), (0,))),
        preferred_element_type=jnp.float32,
    )
    return counts > 0.5


def wanted(every, role):
    owners = every.shape[0] - 2 * HALF

    def asked_from(step):
        return every[HALF + step : HALF + step + owners, HALF - step]

    role = role[:, None]
    before, after = asked_from(-1), asked_from(1)
    even = (role & 1) == 0
    union = asked_from(-2) | asked_from(2) | (even & before) | (~even & after)
    edge = ((role == 0) & before) | ((role == 3) & after)
    beside = (even & after) | (~even & before)
    return union, edge, beside


def body(source_field, weight_blocks, source_ids, target_ids):
    devices = lax.axis_size(AXES)
    n_gy = lax.axis_size("gy")
    me = lax.axis_index(AXES)
    held = weight_blocks.shape[0]
    nb = source_field.shape[0]
    blocks = jnp.arange(nb, dtype=jnp.int32)
    span = 2 * HALF
    ids = jnp.pad(source_ids, (span * held, span * held), constant_values=-(2**20))
    window = lax.dynamic_slice_in_dim(ids, me * held, (2 * span + 1) * held, 0)
    window = window.reshape(2 * span + 1, held)
    sender = me - span + jnp.arange(2 * span + 1, dtype=jnp.int32)[:, None]
    role = (me - HALF + jnp.arange(SPAN, dtype=jnp.int32)) & (QUAD - 1)
    union, edge, beside = wanted(named_blocks(window, sender, nb), role)
    rest = union & ~edge
    sets = jnp.stack([edge, rest, beside]).astype(jnp.bfloat16)
    earlier = (blocks[:, None] < blocks[None, :]).astype(jnp.bfloat16)
    ranks = jnp.einsum("sdb,bc->sdc", sets, earlier, preferred_element_type=jnp.float32).astype(jnp.int32)
    sizes = jnp.sum(sets.astype(jnp.float32), axis=2, keepdims=True).astype(jnp.int32)
    order = jnp.where(
        edge,
        ranks[0],
        jnp.where(rest, sizes[0] + ranks[1], sizes[0] + sizes[1] + blocks[None, :] - ranks[0] - ranks[1]),
    )
    aside = jnp.where(beside, ranks[2], nb)

    r = me & (QUAD - 1)
    partner = HALF + 1 - 2 * (r & 1)
    mine = jnp.concatenate([aside[HALF : HALF + 1], order[HALF : HALF + 1]])
    chosen = jnp.sum(
        jnp.where(mine[:, None, :] == blocks[None, :, None], blocks[None, None, :], 0), axis=2
    )
    sel = jnp.concatenate([chosen[0, :CAP_S], chosen[1]])

    base_a, base_b, base_c, base_h, base_o = 0, nb, 2 * nb, 3 * nb, 3 * nb + CAP_S
    regions = jnp.array(
        [
            [base_b, base_c, base_o, base_h, base_a],
            [base_c, base_h, base_o, base_a, base_b],
            [base_b, base_a, base_o, base_h, base_c],
            [base_a, base_h, base_o, base_c, base_b],
        ],
        jnp.int32,
    )
    region = lax.dynamic_slice_in_dim(regions, r, 1, 0).reshape(SPAN, 1)
    from_partner = lax.dynamic_slice_in_dim(aside, partner, 1, 0)
    table = jnp.where(
        region == base_o, blocks[None, :], jnp.where(region == base_h, from_partner, order)
    )
    table = (region + table).reshape(-1)
    own_src = rows_of(source_ids, me, devices, held)
    low = (me - HALF) * nb
    hits = (own_src - low)[:, None] == jnp.arange(SPAN * nb, dtype=jnp.int32)[None, :]
    place = jnp.sum(jnp.where(hits, table[None, :], 0), axis=1)

    own_tgt = rows_of(target_ids, me, devices, held)
    low = (me - HALF) * TB_DEV
    tgt_asked = named(own_tgt, low, SPAN * TB_DEV).reshape(SPAN, TB_DEV)
    steps = jnp.arange(SPAN, dtype=jnp.int32)[:, None] - HALF
    tgt_group = HALF - jnp.abs(steps)
    tgt_slot = 1 + ranks_of(tgt_asked) + jnp.where(steps > 0, CAP_T, 0)
    hits = (own_tgt - low)[:, None] == jnp.arange(SPAN * TB_DEV, dtype=jnp.int32)[None, :]
    marks = jnp.sum(jnp.where(hits, (tgt_slot + 64 * tgt_group).reshape(-1)[None, :], 0), axis=1)
    group, slot = marks // 64, marks % 64

    index = jnp.arange(held, dtype=jnp.int32)
    groups = jnp.arange(4, dtype=jnp.int32)
    sizes = jnp.sum((group[None, :] == groups[:, None]).astype(jnp.int32), axis=1)
    sizes = (sizes + GROUP - 1) // GROUP * GROUP
    bounds = jnp.sum(jnp.where(groups[None, :] < groups[:, None], sizes[None, :], 0), axis=1)
    earlier = (group[:, None] == group[None, :]) & (index[:, None] < index[None, :])
    position = jnp.sum(earlier.astype(jnp.int32), axis=0)
    position = position + jnp.sum(
        jnp.where(group[None, :] == groups[:, None], bounds[:, None], 0), axis=0
    )
    item = (index * 1024 + place) * 64 + slot
    spots = jnp.arange(held + 4 * GROUP, dtype=jnp.int32)
    packed = jnp.sum(jnp.where(position[None, :] == spots[:, None], item[None, :], 0), axis=1)

    box_asked = []
    for step in range(-HALF, HALF + 1):
        sender = me - step
        valid = (sender >= 0) & (sender < devices)
        rows = rows_of(target_ids, sender, devices, held)
        box_asked.append(named(rows, me * TB_DEV, TB_DEV) & valid)
    box_asked = jnp.stack(box_asked)
    spot = jnp.where(box_asked, ranks_of(box_asked), -1)
    targets = jnp.sum(
        jnp.where(
            spot[:, None, :] == jnp.arange(CAP_T, dtype=jnp.int32)[None, :, None],
            1 + jnp.arange(TB_DEV, dtype=jnp.int32)[None, None, :],
            0,
        ),
        axis=2,
    ).reshape(-1)

    def finish(rare, bounds, packed, sel, targets, source_field, weight_blocks, source_ids):
        sel, bounds, packed, targets = lax.optimization_barrier((sel, bounds, packed, targets))
        pool = exchange_call(n_gy, devices, rare, sel, source_field)
        weights = weight_blocks
        boxes = [None] * SPAN
        below, above = products_call((0,), rare, held, bounds, packed, weights, pool)
        bounds, below, above = lax.optimization_barrier((bounds, below, above))
        boxes[0] = passed_along(below, -2)
        boxes[4] = passed_along(above, 2)
        below, above, own = products_call((1, 2), rare, held, bounds, packed, weights, pool)
        boxes[1] = passed_along(below, -1)
        boxes[3] = passed_along(above, 1)
        boxes[2], source_ids = lax.optimization_barrier((own, source_ids))
        return final_call(targets, boxes), source_ids

    arrays = (bounds, packed, sel, targets, source_field, weight_blocks, source_ids)
    result, late_ids = finish(False, *arrays)
    every = named_blocks(
        late_ids.reshape(devices, held), jnp.arange(devices, dtype=jnp.int32)[:, None], nb
    )
    every = jnp.pad(every, ((HALF, HALF), (0, 0), (0, 0)))
    union, _, _ = wanted(every, jnp.arange(devices, dtype=jnp.int32) % QUAD)
    most = jnp.max(jnp.sum(union.astype(jnp.int32), axis=1))
    return lax.cond(
        most > nb - RARE, lambda result, *arrays: finish(True, *arrays)[0], lambda result, *arrays: result, result, *arrays
    )


def solution(mesh):
    return jax.shard_map(
        body,
        mesh=mesh,
        in_specs=(P(AXES, None, None), P(AXES, None, None), P(), P()),
        out_specs=P(AXES, None, None),
        check_vma=False,
    )
```
